256 devices in a mesh: groups: 4 (over y, x), gx: 64 (over z, core).
Axes of the slice: x: 2, y: 2, z: 32, core: 2. Of those that a mesh axis runs over, the one named last changes fastest.
The devices are a block of a 4x8x32 slice.
Arguments:
- tokens: bfloat16 [1536, 4608], P('groups', 'gx'), parts along dimension 0, may hold values from -6 to 6
- gate_weight: bfloat16 [64, 576, 2304], P('gx'), may hold values from -0.09375 to 0.09375
- up_weight: bfloat16 [64, 576, 2304], P('gx'), may hold values from -0.09375 to 0.09375
- down_weight: bfloat16 [64, 2304, 576], P('gx'), may hold values from -0.046875 to 0.046875
Outputs:
- mixed: bfloat16 [1536, 4608], P('groups', 'gx'), parts along dimension 0
The draws below stay inside these ranges and needn't reach their ends.
There are 4 independent parts, one for each index of `groups`. The reference program is written for one: setup_inputs(seed, part) draws one part's arguments, and reference() takes and returns one part's arrays. A program takes and returns all parts, laid end to end along the dimension named above; an argument that names none is the same for every part. Nothing has to cross between parts.
All inputs are finite; a program needn't handle non-finite values.
Results may differ from the reference program's by a relative error of at most 0.015.
Values may be sent and summed in bfloat16 or wider, within the bound.
No kernel may reach another device: no remote copies, remote signals or barrier semaphores. Data moves between devices by JAX's collectives and lax.ppermute only.
A program may use at most 128 MiB of HBM per device.

```python
import jax
import jax.numpy as jnp

D = 4608
FF = 18432
TOK = 384
XS = 8
YS = 8


def level_of(own_key, shape, cuts, smallest, top_value):
    gain = 1.0
    for position, parts in cuts:
        draws = jax.random.uniform(jax.random.fold_in(jax.random.fold_in(own_key, 6), position), (parts,), jnp.float32, smallest / len(cuts), top_value / len(cuts))
        gain = gain * jnp.repeat(jnp.exp(draws), shape[position] // parts).reshape((-1,) + (1,) * (len(shape) - 1 - position))
    return gain


def scatter_about(rng, shape, spread, reach, cuts=(), kind=jnp.bfloat16):
    result = spread * jax.random.normal(rng, shape, jnp.float32)
    if cuts:
        result = result * level_of(rng, shape, cuts, -0.22, 0.18)
    return jnp.clip(result, -reach, reach).astype(kind)


def setup_inputs(seed: int = 0, part: int = 0) -> dict:
    splits = jax.random.split(jax.random.key(seed), 5)
    part_splits = jax.random.split(jax.random.fold_in(splits[4], part), 5)
    tokens = scatter_about(part_splits[0], (TOK, D), 1.0, 6.0, ((1, 64),))
    gate_weight = scatter_about(splits[1], (XS * YS, D // XS, FF // YS), D ** -0.5, 0.09375, ((0, 64),))
    up_weight = scatter_about(splits[2], (XS * YS, D // XS, FF // YS), D ** -0.5, 0.09375, ((0, 64),))
    down_weight = scatter_about(splits[3], (XS * YS, FF // XS, D // YS), FF ** -0.5, 0.046875, ((0, 64),))
    return {"tokens": tokens, "gate_weight": gate_weight, "up_weight": up_weight, "down_weight": down_weight}


def assemble(tile_stack, row_count, column_count):
    blocks = tile_stack.reshape(YS, XS, YS, -1, tile_stack.shape[2])
    return blocks.transpose(2, 1, 3, 0, 4).reshape(row_count, column_count)


def reference(tokens, gate_weight, up_weight, down_weight):
    gate_full = assemble(gate_weight, D, FF)
    up_full = assemble(up_weight, D, FF)
    down_full = assemble(down_weight, FF, D)
    gate = jnp.dot(tokens, gate_full, preferred_element_type=jnp.float32)
    up_proj = jnp.dot(tokens, up_full, preferred_element_type=jnp.float32)
    hidden = (jax.nn.gelu(gate, approximate=True) * up_proj).astype(jnp.bfloat16)
    mixed = jnp.dot(hidden, down_full, preferred_element_type=jnp.float32)
    return mixed.astype(jnp.bfloat16)
```

```python
import jax
import jax.numpy as jnp
from jax import lax
from jax.sharding import PartitionSpec as P

XS = 8
CHUNK = 128
SQRT_2_OVER_PI = 0.7978845608


def ring_route(axis, right, left):
    count = lax.axis_size(axis)
    return [(i, (i + (left if i & 1 else right)) % count) for i in range(count)]


def partner_route(axis, bit):
    return [(i, i ^ (1 << bit)) for i in range(lax.axis_size(axis))]


def pick(pair, which, axis):
    return lax.dynamic_index_in_dim(pair, which, axis, keepdims=False)


def halve(value, axis, bit, which):
    outgoing = pick(value, 1 - which, axis).astype(jnp.bfloat16)
    kept = pick(value, which, axis)
    arrived = lax.ppermute(outgoing, "gx", partner_route("gx", bit))
    return kept + arrived.astype(jnp.float32)


def shards(tokens, gate_weight, up_weight, down_weight):
    index = lax.axis_index("gx")
    segments = lax.axis_size("gx") // XS
    segment = index // XS
    core = index & 1
    near = index >> 1 & 1
    far = index >> 2 & 1
    half_way = segments // 2
    both = ring_route("gx", XS, -XS)

    own = tokens.T
    features, count = own.shape
    joined = jnp.zeros((segments, features, count), own.dtype)

    def put(buffer, block, where):
        return lax.dynamic_update_index_in_dim(buffer, block, where % segments, 0)

    joined = put(joined, own, segment)
    right = left = own
    for step in range(1, half_way):
        right = lax.ppermute(right, "gx", ring_route("gx", XS, XS))
        left = lax.ppermute(left, "gx", ring_route("gx", -XS, -XS))
        joined = put(joined, right, segment - step + segments)
        joined = put(joined, left, segment + step)
    last = lax.ppermute(jnp.where(core == 0, right, left), "gx", both)
    joined = put(joined, last, segment + half_way)
    joined = joined.reshape(segments * features, count)

    contract = (((0,), (0,)), ((), ()))
    outputs = []
    for first in range(0, count, CHUNK):
        part = joined[:, first : first + CHUNK]
        gate = lax.dot_general(gate_weight[0], part, contract, preferred_element_type=jnp.float32)
        up = lax.dot_general(up_weight[0], part, contract, preferred_element_type=jnp.float32)
        width = gate.shape[0] // XS
        value = jnp.stack([gate, up]).reshape(2, 2, 2, 2, width, CHUNK)
        value = halve(value, 3, 0, core)
        value = halve(value, 2, 1, near)
        value = halve(value, 1, 2, far)
        hidden = (jax.nn.gelu(value[0], approximate=True) * value[1]).astype(jnp.bfloat16)
        other = lax.ppermute(hidden, "gx", partner_route("gx", 0))
        block = jnp.where(
            core == 0, jnp.stack([hidden, other]), jnp.stack([other, hidden])
        )
        gathered = jnp.zeros((segments, width, CHUNK), jnp.bfloat16)
        gathered = put(gathered, hidden, segment)
        turn = 1 - 2 * core
        for step in range(1, half_way):
            block = lax.ppermute(block, "gx", both)
            crossed = lax.ppermute(pick(block, 1 - core, 0), "gx", partner_route("gx", 0))
            gathered = put(gathered, pick(block, core, 0), segment - turn * step + segments)
            gathered = put(gathered, crossed, segment + turn * step + segments)
        last = lax.ppermute(pick(block, core, 0), "gx", both)
        gathered = put(gathered, last, segment + half_way)
        result = lax.dot_general(
            down_weight[0],
            gathered.reshape(segments * width, CHUNK),
            contract,
            preferred_element_type=jnp.float32,
        )
        result = result.reshape(2, 2, 2, result.shape[0] // XS, CHUNK)
        result = halve(result, 2, 0, core)
        result = halve(result, 1, 1, near)
        result = halve(result, 0, 2, far)
        outputs.append(result.astype(jnp.bfloat16))
    return jnp.concatenate(outputs, 1).T


def solution(mesh):
    placed = (P("groups", "gx"), P("gx", None, None), P("gx", None, None), P("gx", None, None))
    return jax.shard_map(
        shards, mesh=mesh, in_specs=placed, out_specs=P("groups", "gx"), check_vma=False
    )
```

```python
import jax
import jax.numpy as jnp
from jax import lax
from jax.experimental.layout import Layout, with_layout_constraint
from jax.sharding import PartitionSpec as P

XS = 8
CHUNK = 128


def ring_route(axis, right, left):
    count = lax.axis_size(axis)
    return [(i, (i + (left if i & 1 else right)) % count) for i in range(count)]


def partner_route(axis, bit):
    return [(i, i ^ (1 << bit)) for i in range(lax.axis_size(axis))]


def pick(pair, which, axis):
    return lax.dynamic_index_in_dim(pair, which, axis, keepdims=False)


def after(value, *earlier):
    return lax.optimization_barrier((value, *earlier))[0]


def halve_send(value, axis, bit, which):
    outgoing = pick(value, 1 - which, axis).astype(jnp.bfloat16)
    return pick(value, which, axis), lax.ppermute(outgoing, "gx", partner_route("gx", bit))


def add(kept, arrived):
    return kept + arrived.astype(jnp.float32)


def shards(tokens, gate_weight, up_weight, down_weight):
    index = lax.axis_index("gx")
    segments = lax.axis_size("gx") // XS
    segment = index // XS
    core = index & 1
    near = index >> 1 & 1
    far = index >> 2 & 1
    half_way = segments // 2
    both = ring_route("gx", XS, -XS)

    count, features = tokens.shape
    joined = jnp.zeros((count, segments, features), tokens.dtype)

    def put(buffer, block, where):
        return lax.dynamic_update_index_in_dim(buffer, block, where % segments, 1)

    joined = put(joined, tokens, segment)
    right = left = tokens
    for step in range(1, half_way):
        right = lax.ppermute(right, "gx", ring_route("gx", XS, XS))
        left = lax.ppermute(left, "gx", ring_route("gx", -XS, -XS))
        joined = put(joined, right, segment - step + segments)
        joined = put(joined, left, segment + step)
    last = lax.ppermute(jnp.where(core == 0, right, left), "gx", both)
    joined = put(joined, last, segment + half_way)
    joined = joined.reshape(count, segments * features)

    t_minor = Layout(major_to_minor=(1, 0))
    parts = []
    for weight in (gate_weight, up_weight):
        part = jnp.dot(joined, weight[0], preferred_element_type=jnp.float32)
        parts.append(with_layout_constraint(part, t_minor))
    width = parts[0].shape[1] // XS

    chunks = range(count // CHUNK)
    stage = []
    for c in chunks:
        kept, outgoing = [], []
        for part in parts:
            piece = part[CHUNK * c : CHUNK * c + CHUNK].reshape(CHUNK, 2, 2, 2, width)
            kept.append(pick(piece, core, 3))
            outgoing.append(pick(piece, 1 - core, 3).astype(jnp.bfloat16))
        arrived = lax.ppermute(jnp.stack(outgoing), "gx", partner_route("gx", 0))
        value = jnp.stack(kept) + arrived.astype(jnp.float32)
        stage.append(halve_send(value, 3, 1, near))
    hidden, block = [], []
    for c in chunks:
        kept, arrived = stage[c]
        if c == len(chunks) - 1 and hidden:
            arrived = after(arrived, hidden[0])
        kept, arrived = halve_send(add(kept, arrived), 2, 2, far)
        if block:
            arrived = after(arrived, block[-1])
        value = add(kept, arrived)
        hidden.append((jax.nn.gelu(value[0], approximate=True) * value[1]).astype(jnp.bfloat16))
        other = lax.ppermute(hidden[c], "gx", partner_route("gx", 0))
        block.append(
            jnp.where(core == 0, jnp.stack([hidden[c], other]), jnp.stack([other, hidden[c]]))
        )
    turn = 1 - 2 * core
    rounds = [block]
    for step in range(1, half_way):
        rounds.append([lax.ppermute(b, "gx", both) for b in rounds[-1]])
    last = [lax.ppermute(pick(b, core, 0), "gx", both) for b in rounds[-1]]
    results = []
    for c in chunks:
        gathered = jnp.zeros((CHUNK, segments, width), jnp.bfloat16)
        gathered = put(gathered, hidden[c], segment)
        here = jnp.stack([rounds[step][c] for step in range(1, half_way)])
        crossed = lax.ppermute(pick(here, 1 - core, 1), "gx", partner_route("gx", 0))
        for step in range(1, half_way):
            mine = pick(rounds[step][c], core, 0)
            gathered = put(gathered, mine, segment - turn * step + segments)
            gathered = put(gathered, crossed[step - 1], segment + turn * step + segments)
        gathered = put(gathered, last[c], segment + half_way)
        result = jnp.dot(
            gathered.reshape(CHUNK, segments * width),
            down_weight[0],
            preferred_element_type=jnp.float32,
        )
        results.append(result)
    result = jnp.concatenate(results, 0).reshape(count, 2, 2, 2, features)
    result = add(*halve_send(result, 3, 0, core))
    result = add(*halve_send(result, 2, 1, near))
    result = add(*halve_send(result, 1, 2, far))
    return result.astype(jnp.bfloat16)


def solution(mesh):
    placed = (P("groups", "gx"), P("gx", None, None), P("gx", None, None), P("gx", None, None))
    return jax.shard_map(
        shards, mesh=mesh, in_specs=placed, out_specs=P("groups", "gx"), check_vma=False
    )
```
